32 devices in a mesh: ep: 2 (over core), fsdp: 16 (over z, y, x).
Axes of the slice: x: 2, y: 2, z: 4, core: 2. Of those that a mesh axis runs over, the one named last changes fastest.
Arguments:
- train_down: float32 [8, 14336, 4096], P('ep', None, 'fsdp'), may hold values from -0.0625 to 0.0625
- router_weight: float32 [4096, 8], P('fsdp', 'ep'), may hold values from -0.09375 to 0.09375
- router_gain: float32 [4096], P('fsdp'), may hold values from 0.25 to 1.75
Outputs:
- ready_down: bfloat16 [8, 14336, 4096], P('ep', 'fsdp')
- scale_down: float32 [8, 14336], P('ep', 'fsdp')
- serve_router: bfloat16 [4096, 8], replicated
The draws below stay inside these ranges and needn't reach their ends.
All inputs are finite; a program needn't handle non-finite values.
Results may differ from the reference program's by a relative error of at most 0.001.
Values may be sent and summed in bfloat16 or wider, within the bound.
A program may use at most 192 MiB of HBM per device.

```python
import jax
import jax.numpy as jnp
from jax import lax

EXPERTS = 8
D_MODEL = 4096
D_EXPERT = 14336


def strengthened(values, stream_key, source, target, shards_of, factor):
    def block_of(position):
        return (jnp.arange(values.shape[position]) // (values.shape[position] // shards_of)).reshape((-1,) + (1,) * (values.ndim - 1 - position))

    first = jax.random.permutation(stream_key, shards_of)[block_of(target)]
    far = (block_of(target) + shards_of // 2) % shards_of
    return jnp.where((block_of(source) == first) | (block_of(source) == far), factor * values, values)


def steps_of(key, shape, shards, smallest, top_value):
    level, own = 1.0, jax.random.fold_in(key, 6)
    for position, parts in shards:
        steps = jnp.exp(jax.random.uniform(jax.random.fold_in(own, position), (parts,), jnp.float32, smallest / len(shards), top_value / len(shards)))
        level = level * jnp.repeat(steps, shape[position] // parts).reshape([-1 if axis == position else 1 for axis in range(len(shape))])
    return level


def gaussian(stream_key, dims, width, limit, cuts=(), held_as=jnp.bfloat16):
    array = jax.random.normal(stream_key, dims, jnp.float32) * width
    if len(cuts) > 0:
        array = steps_of(stream_key, dims, cuts, -0.22, 0.18) * array
    return jnp.clip(array, min=-limit, max=limit).astype(held_as)


def heavy_noise(own_key, dims, deviation, most, shards, heavy, dtype=jnp.bfloat16):
    drawn = deviation * jax.random.normal(own_key, dims, jnp.float32)
    if shards:
        drawn = drawn * steps_of(own_key, dims, shards, -0.22, 0.18)
    return jnp.clip(strengthened(drawn, jax.random.fold_in(own_key, 3), *heavy), -most, most).astype(dtype)


def setup_inputs(seed: int = 0) -> dict:
    arg_keys = jax.random.split(jax.random.key(seed), 4)
    train_down = heavy_noise(arg_keys[0], (EXPERTS, D_EXPERT, D_MODEL), D_EXPERT ** -0.5, 0.0625, ((0, 2), (2, 16)), (2, 1, 16, 2.0), jnp.float32)
    router_weight = gaussian(arg_keys[1], (D_MODEL, EXPERTS), D_MODEL ** -0.5, 0.09375, ((0, 16), (1, 2)), jnp.float32)
    router_gain = jnp.clip(1.0 + 0.15 * jax.random.normal(arg_keys[2], (D_MODEL,), jnp.float32), 0.25, 1.75)
    return {"train_down": train_down, "router_weight": router_weight, "router_gain": router_gain}


def reference(train_down, router_weight, router_gain):
    scale_down = jnp.sqrt(lax.optimization_barrier(jnp.sum(train_down * train_down, axis=2)))
    ready_down = (train_down / jnp.expand_dims(scale_down, 2)).astype(jnp.bfloat16)
    serve_router = (router_weight * router_gain[:, None]).astype(jnp.bfloat16)
    return (ready_down, scale_down, serve_router)
```

```python
import functools

import jax
import jax.numpy as jnp
from jax import lax
from jax.experimental import pallas as pl
from jax.experimental.pallas import tpu as pltpu
from jax.sharding import PartitionSpec as P

MESH = pl.DeviceIdType.MESH
BUFFERS = 4


def kernel(n, g, w_ref, part_ref, ready_ref, scale_ref, router_ref, wbuf, stage, sums, wide, sent, got, inv, gathered,
           wsem, send, recv, rs_send, rs_recv, ag_send, ag_recv, ro_send, ro_recv, ro_own):
    experts, _, width = w_ref.shape
    rows = stage.shape[1]
    blocks = experts * n
    chunk = 64 if rows % 64 == 0 else 8
    lanes = sums.shape[1]
    me, group = lax.axis_index("fsdp"), lax.axis_index("ep")
    flat = group * n + me
    everyone = g * n

    def device(index):
        return {"ep": index // n, "fsdp": index % n}

    def partner(k):
        if n & (n - 1):
            return (me + k) % n
        found, bit = 0, 1
        while bit < n:
            found = found + (((me // bit) % 2 + (k // bit) % 2) % 2) * bit
            bit *= 2
        return found

    def distance(t):
        j = t % n
        return n - 1 - j // 2 - (j % 2) * (n // 2)

    def load(expert, owner, slot):
        return pltpu.make_async_copy(w_ref.at[expert, pl.ds(owner * rows, rows), :], wbuf.at[slot], wsem.at[slot])

    def load_sum(t):
        return load(t % experts, t // experts, t % BUFFERS)

    def load_scale(t):
        return load(t // n, partner(distance(t)), t % BUFFERS)

    for t in range(min(BUFFERS - 1, blocks)):
        load_sum(t).start()

    barrier = pltpu.get_barrier_semaphore()

    @pl.loop(1, everyone)
    def _(q):
        pl.semaphore_signal(barrier, inc=1, device_id=device((flat + q) % everyone), device_id_type=MESH)

    pl.semaphore_wait(barrier, everyone - 1)

    def router_copy(q):
        return pltpu.make_async_remote_copy(
            src_ref=part_ref, dst_ref=router_ref.at[group, me], send_sem=ro_send.at[q], recv_sem=ro_recv.at[q],
            device_id=device((flat + q) % everyone), device_id_type=MESH)

    own_router = pltpu.make_async_copy(part_ref, router_ref.at[group, me], ro_own)
    own_router.start()

    sums[...] = jnp.zeros_like(sums)

    @pl.loop(0, blocks)
    def _(t):
        @pl.when(t + BUFFERS - 1 < blocks)
        def _():
            load_sum(t + BUFFERS - 1).start()

        load_sum(t).wait()
        slot = t % BUFFERS

        @pl.loop(0, rows // chunk)
        def _(c):
            at = pl.ds(pl.multiple_of(c * chunk, chunk), chunk)
            x = wbuf[slot, at, :]
            total = jnp.sum(x * x, axis=1, keepdims=True)
            lane = lax.broadcasted_iota(jnp.int32, (chunk, lanes), 1)
            sums[at, :] = jnp.where(lane == t, total, sums[at, :])

    for t in range(min(BUFFERS - 1, blocks)):
        load_scale(t).start()

    wide[...] = sums[...].T
    for d in range(n):
        sent[d] = wide[d * experts:(d + 1) * experts, :]

    def scatter_copy(k):
        other = partner(k)
        return pltpu.make_async_remote_copy(
            src_ref=sent.at[other], dst_ref=got.at[k], send_sem=rs_send.at[k], recv_sem=rs_recv.at[k],
            device_id={"fsdp": other}, device_id_type=MESH)

    def gather_copy(k):
        return pltpu.make_async_remote_copy(
            src_ref=inv, dst_ref=gathered.at[me], send_sem=ag_send.at[k], recv_sem=ag_recv.at[k],
            device_id={"fsdp": partner(k)}, device_id_type=MESH)

    @pl.loop(1, n)
    def _(k):
        scatter_copy(n - k).start()

    total = sent[me]
    got[0] = total
    for k in range(1, n):
        scatter_copy(k).wait_recv()
        total = total + got[k]
    scale = jnp.sqrt(total)
    scale_ref[...] = scale
    inv[...] = 1.0 / scale
    gathered[me] = inv[...]

    @pl.loop(1, n)
    def _(k):
        gather_copy(n - k).start()

    @pl.loop(1, n)
    def _(k):
        gather_copy(k).wait_recv()

    for d in range(n):
        wide[d * experts:(d + 1) * experts, :] = gathered[d]
    sums[...] = wide[...].T

    def piece(t):
        return ready_ref.at[t // n, :, pl.ds(pl.multiple_of(me * width, width), width)]

    def send_copy(t):
        return pltpu.make_async_remote_copy(
            src_ref=stage.at[t], dst_ref=piece(t), send_sem=send.at[t], recv_sem=recv.at[t],
            device_id={"fsdp": partner(distance(t))}, device_id_type=MESH)

    def keep_copy(t):
        return pltpu.make_async_copy(stage.at[t], piece(t), send.at[t])

    def issue(t):
        @pl.when(t % n != n - 1)
        def _():
            send_copy(t).start()

        @pl.when(t % n == n - 1)
        def _():
            keep_copy(t).start()

    @pl.loop(0, blocks)
    def _(t):
        @pl.when(t + BUFFERS - 1 < blocks)
        def _():
            load_scale(t + BUFFERS - 1).start()

        load_scale(t).wait()
        slot = t % BUFFERS
        column = partner(distance(t)) * experts + t // n

        @pl.loop(0, rows // chunk)
        def _(c):
            at = pl.ds(pl.multiple_of(c * chunk, chunk), chunk)
            lane = lax.broadcasted_iota(jnp.int32, (chunk, lanes), 1)
            factor = jnp.sum(jnp.where(lane == column, sums[at, :], 0.0), axis=1, keepdims=True)
            stage[t, at, :] = (wbuf[slot, at, :] * factor).astype(jnp.bfloat16)

        @pl.when(t > 0)
        def _():
            issue(t - 1)

    issue(blocks - 1)

    @pl.loop(1, everyone)
    def _(q):
        router_copy(q).start()

    @pl.loop(1, n)
    def _(k):
        scatter_copy(k).wait_send()
        gather_copy(k).wait_send()

    @pl.loop(0, blocks)
    def _(t):
        @pl.when(t % n != n - 1)
        def _():
            send_copy(t).wait_send()
            send_copy(t).wait_recv()

        @pl.when(t % n == n - 1)
        def _():
            keep_copy(t).wait()

    @pl.loop(1, everyone)
    def _(q):
        router_copy(q).wait_send()
        router_copy(q).wait_recv()

    own_router.wait()


def body(n, g, train_down, router_weight, router_gain):
    experts, length, width = train_down.shape
    rows, blocks = length // n, experts * n
    lanes = -(-blocks // 128) * 128
    part = (router_weight * router_gain[:, None]).astype(jnp.bfloat16).astype(jnp.float32).T
    dma = pltpu.SemaphoreType.DMA
    vmem = pl.BlockSpec(memory_space=pltpu.VMEM)
    hbm = pl.BlockSpec(memory_space=pl.ANY)
    ready, scale, router = pl.pallas_call(
        functools.partial(kernel, n, g),
        out_shape=(
            jax.ShapeDtypeStruct((experts, rows, n * width), jnp.bfloat16),
            jax.ShapeDtypeStruct((experts, rows), jnp.float32),
            jax.ShapeDtypeStruct((g, n) + part.shape, jnp.float32),
        ),
        in_specs=[hbm, vmem],
        out_specs=(hbm, vmem, hbm),
        scratch_shapes=[
            pltpu.VMEM((BUFFERS, rows, width), jnp.float32),
            pltpu.VMEM((blocks, rows, width), jnp.bfloat16),
            pltpu.VMEM((rows, lanes), jnp.float32),
            pltpu.VMEM((lanes, rows), jnp.float32),
            pltpu.VMEM((n, experts, rows), jnp.float32),
            pltpu.VMEM((n, experts, rows), jnp.float32),
            pltpu.VMEM((experts, rows), jnp.float32),
            pltpu.VMEM((n, experts, rows), jnp.float32),
            dma((BUFFERS,)),
            dma((blocks,)),
            dma((blocks,)),
            dma((n,)),
            dma((n,)),
            dma((n,)),
            dma((n,)),
            dma((n * g,)),
            dma((n * g,)),
            dma,
        ],
        compiler_params=pltpu.CompilerParams(collective_id=0, has_side_effects=True, vmem_limit_bytes=60 * 2**20),
    )(train_down, part)
    router = router.transpose(1, 3, 0, 2).reshape(n * part.shape[1], g * experts)
    return ready, scale, router.astype(jnp.bfloat16)


def solution(mesh):
    placed = (P("ep", None, "fsdp"), P("fsdp", "ep"), P("fsdp"))
    return jax.shard_map(
        functools.partial(body, mesh.shape["fsdp"], mesh.shape["ep"]),
        mesh=mesh,
        in_specs=placed,
        out_specs=(P("ep", "fsdp", None), P("ep", "fsdp"), P()),
        check_vma=False,
    )
```

```python
import functools

import jax
import jax.numpy as jnp
from jax import lax
from jax.experimental import pallas as pl
from jax.experimental.pallas import tpu as pltpu
from jax.sharding import PartitionSpec as P

MESH = pl.DeviceIdType.MESH
BUFFERS = 4


def kernel(n, g, w_ref, part_ref, ready_ref, scale_ref, router_ref, wbuf, stage, sums, wide, sent, got, inv, gathered,
           wsem, send, recv, rs_send, rs_recv, ag_send, ag_recv, ro_send, ro_recv, ro_own):
    experts, _, width = w_ref.shape
    rows = stage.shape[1]
    blocks = experts * n
    chunk = 64 if rows % 64 == 0 else 8
    lanes = sums.shape[1]
    me, group = lax.axis_index("fsdp"), lax.axis_index("ep")
    flat = group * n + me
    everyone = g * n

    def device(index):
        return {"ep": index // n, "fsdp": index % n}

    def partner(k):
        if n & (n - 1):
            return (me + k) % n
        found, bit = 0, 1
        while bit < n:
            found = found + (((me // bit) % 2 + (k // bit) % 2) % 2) * bit
            bit *= 2
        return found

    def distance(t):
        j = t % n
        return n - 1 - j // 2 - (j % 2) * (n // 2)

    def load(expert, owner, slot):
        return pltpu.make_async_copy(w_ref.at[expert, pl.ds(owner * rows, rows), :], wbuf.at[slot], wsem.at[slot])

    def load_sum(t):
        return load(t % experts, t // experts, t % BUFFERS)

    def load_scale(t):
        return load(t // n, partner(distance(t)), t % BUFFERS)

    for t in range(min(BUFFERS - 1, blocks)):
        load_sum(t).start()

    barrier = pltpu.get_barrier_semaphore()

    @pl.loop(1, everyone)
    def _(q):
        pl.semaphore_signal(barrier, inc=1, device_id=device((flat + q) % everyone), device_id_type=MESH)

    pl.semaphore_wait(barrier, everyone - 1)

    def router_copy(q):
        return pltpu.make_async_remote_copy(
            src_ref=part_ref, dst_ref=router_ref.at[group, me], send_sem=ro_send.at[q], recv_sem=ro_recv.at[q],
            device_id=device((flat + q) % everyone), device_id_type=MESH)

    own_router = pltpu.make_async_copy(part_ref, router_ref.at[group, me], ro_own)
    own_router.start()

    sums[...] = jnp.zeros_like(sums)

    @pl.loop(0, blocks)
    def _(t):
        @pl.when(t + BUFFERS - 1 < blocks)
        def _():
            load_sum(t + BUFFERS - 1).start()

        load_sum(t).wait()
        slot = t % BUFFERS

        @pl.loop(0, rows // chunk)
        def _(c):
            at = pl.ds(pl.multiple_of(c * chunk, chunk), chunk)
            x = wbuf[slot, at, :]
            total = jnp.sum(x * x, axis=1, keepdims=True)
            lane = lax.broadcasted_iota(jnp.int32, (chunk, lanes), 1)
            sums[at, :] = jnp.where(lane == t, total, sums[at, :])

    for t in range(min(BUFFERS - 1, blocks)):
        load_scale(t).start()

    wide[...] = sums[...].T
    for d in range(n):
        sent[d] = wide[d * experts:(d + 1) * experts, :]

    def scatter_copy(k):
        other = partner(k)
        return pltpu.make_async_remote_copy(
            src_ref=sent.at[other], dst_ref=got.at[k], send_sem=rs_send.at[k], recv_sem=rs_recv.at[k],
            device_id={"fsdp": other}, device_id_type=MESH)

    def gather_copy(k):
        return pltpu.make_async_remote_copy(
            src_ref=inv, dst_ref=gathered.at[me], send_sem=ag_send.at[k], recv_sem=ag_recv.at[k],
            device_id={"fsdp": partner(k)}, device_id_type=MESH)

    @pl.loop(1, n)
    def _(k):
        scatter_copy(n - k).start()

    total = sent[me]
    got[0] = total
    for k in range(1, n):
        scatter_copy(k).wait_recv()
        total = total + got[k]
    scale = jnp.sqrt(total)
    scale_ref[...] = scale
    inv[...] = 1.0 / scale
    gathered[me] = inv[...]

    @pl.loop(1, n)
    def _(k):
        gather_copy(n - k).start()

    @pl.loop(1, n)
    def _(k):
        gather_copy(k).wait_recv()

    for d in range(n):
        wide[d * experts:(d + 1) * experts, :] = gathered[d]
    sums[...] = wide[...].T

    def piece(t):
        return ready_ref.at[t // n, me]

    def send_copy(t):
        return pltpu.make_async_remote_copy(
            src_ref=stage.at[t], dst_ref=piece(t), send_sem=send.at[t], recv_sem=recv.at[t],
            device_id={"fsdp": partner(distance(t))}, device_id_type=MESH)

    def keep_copy(t):
        return pltpu.make_async_copy(stage.at[t], piece(t), send.at[t])

    def issue(t):
        @pl.when(t % n != n - 1)
        def _():
            send_copy(t).start()

        @pl.when(t % n == n - 1)
        def _():
            keep_copy(t).start()

    @pl.loop(0, blocks)
    def _(t):
        @pl.when(t + BUFFERS - 1 < blocks)
        def _():
            load_scale(t + BUFFERS - 1).start()

        load_scale(t).wait()
        slot = t % BUFFERS
        column = partner(distance(t)) * experts + t // n

        @pl.loop(0, rows // chunk)
        def _(c):
            at = pl.ds(pl.multiple_of(c * chunk, chunk), chunk)
            lane = lax.broadcasted_iota(jnp.int32, (chunk, lanes), 1)
            factor = jnp.sum(jnp.where(lane == column, sums[at, :], 0.0), axis=1, keepdims=True)
            stage[t, at, :] = (wbuf[slot, at, :] * factor).astype(jnp.bfloat16)

        @pl.when(t > 0)
        def _():
            issue(t - 1)

    issue(blocks - 1)

    @pl.loop(1, everyone)
    def _(q):
        router_copy(q).start()

    @pl.loop(1, n)
    def _(k):
        scatter_copy(k).wait_send()
        gather_copy(k).wait_send()

    @pl.loop(0, blocks)
    def _(t):
        @pl.when(t % n != n - 1)
        def _():
            send_copy(t).wait_send()
            send_copy(t).wait_recv()

        @pl.when(t % n == n - 1)
        def _():
            keep_copy(t).wait()

    @pl.loop(1, everyone)
    def _(q):
        router_copy(q).wait_send()
        router_copy(q).wait_recv()

    own_router.wait()


def join_kernel(pieces_ref, joined_ref):
    n, width = pieces_ref.shape[1], pieces_ref.shape[3]
    for d in range(n):
        joined_ref[0, :, d * width:(d + 1) * width] = pieces_ref[0, d]


def join(pieces):
    experts, n, rows, width = pieces.shape
    tile = next(size for size in (128, 64, rows) if rows % size == 0)
    return pl.pallas_call(
        join_kernel,
        grid=(experts, rows // tile),
        in_specs=[pl.BlockSpec((1, n, tile, width), lambda e, r: (e, 0, r, 0))],
        out_specs=pl.BlockSpec((1, tile, n * width), lambda e, r: (e, r, 0)),
        out_shape=jax.ShapeDtypeStruct((experts, rows, n * width), pieces.dtype),
    )(pieces)


def body(n, g, train_down, router_weight, router_gain):
    experts, length, width = train_down.shape
    rows, blocks = length // n, experts * n
    lanes = -(-blocks // 128) * 128
    part = (router_weight * router_gain[:, None]).astype(jnp.bfloat16).astype(jnp.float32).T
    dma = pltpu.SemaphoreType.DMA
    vmem = pl.BlockSpec(memory_space=pltpu.VMEM)
    hbm = pl.BlockSpec(memory_space=pl.ANY)
    ready, scale, router = pl.pallas_call(
        functools.partial(kernel, n, g),
        out_shape=(
            jax.ShapeDtypeStruct((experts, n, rows, width), jnp.bfloat16),
            jax.ShapeDtypeStruct((experts, rows), jnp.float32),
            jax.ShapeDtypeStruct((g, n) + part.shape, jnp.float32),
        ),
        in_specs=[hbm, vmem],
        out_specs=(hbm, vmem, hbm),
        scratch_shapes=[
            pltpu.VMEM((BUFFERS, rows, width), jnp.float32),
            pltpu.VMEM((blocks, rows, width), jnp.bfloat16),
            pltpu.VMEM((rows, lanes), jnp.float32),
            pltpu.VMEM((lanes, rows), jnp.float32),
            pltpu.VMEM((n, experts, rows), jnp.float32),
            pltpu.VMEM((n, experts, rows), jnp.float32),
            pltpu.VMEM((experts, rows), jnp.float32),
            pltpu.VMEM((n, experts, rows), jnp.float32),
            dma((BUFFERS,)),
            dma((blocks,)),
            dma((blocks,)),
            dma((n,)),
            dma((n,)),
            dma((n,)),
            dma((n,)),
            dma((n * g,)),
            dma((n * g,)),
            dma,
        ],
        compiler_params=pltpu.CompilerParams(collective_id=0, has_side_effects=True, vmem_limit_bytes=60 * 2**20),
    )(train_down, part)
    router = router.transpose(1, 3, 0, 2).reshape(n * part.shape[1], g * experts)
    return join(ready), scale, router.astype(jnp.bfloat16)


def solution(mesh):
    placed = (P("ep", None, "fsdp"), P("fsdp", "ep"), P("fsdp"))
    return jax.shard_map(
        functools.partial(body, mesh.shape["fsdp"], mesh.shape["ep"]),
        mesh=mesh,
        in_specs=placed,
        out_specs=(P("ep", "fsdp", None), P("ep", "fsdp"), P()),
        check_vma=False,
    )
```
